32 devices in a mesh: groups: 2 (over y), blk: 4 (over z), cols: 2 (over x), sub: 2 (over core).
Axes of the slice: x: 2, y: 2, z: 4, core: 2. Of those that a mesh axis runs over, the one named last changes fastest.
Arguments:
- features: bfloat16 [4096, 256], P(('groups', 'blk', 'cols'), 'sub'), parts along dimension 0, may hold values from -60 to 60, as said below
- vector: float32 [4096], P(('groups', 'blk', 'cols')), parts along dimension 0, may hold values from 0.1 to 100, as said below
Outputs:
- new_vector: float32 [4096], P(('groups', 'blk', 'cols')), parts along dimension 0
- mean_affinity: float32 [4096], P(('groups', 'blk', 'cols')), parts along dimension 0
The draws below stay inside these ranges and needn't reach their ends.
There are 2 independent parts, one for each index of `groups`. The reference program is written for one: setup_inputs(seed, part) draws one part's arguments, and reference() takes and returns one part's arrays. A program takes and returns all parts, laid end to end along the dimension named above; each array names one. Nothing has to cross between parts.
Inputs may be any that keep to these rules, and one draw needn't show every extreme that they name: Real-valued features; no row is zero. `vector`: positive entries.
All inputs are finite; a program needn't handle non-finite values. Where the reference program divides by a largest or mean magnitude, that divisor is 1e-20 or more.
Results may differ from the reference program's by a relative error of at most 0.0033.
Values may be sent and summed in bfloat16 or wider, within the bound.
No kernel may reach another device: no remote copies, remote signals or barrier semaphores. Data moves between devices by JAX's collectives and lax.ppermute only.
A program may use at most 64 MiB of HBM per device.

```python
import math
import jax
import jax.numpy as jnp
from jax import lax

F = 256
POWER = 16
POINTS = 2048
CLUSTERS = 64


def draw_features(key, part):
    base = jax.random.fold_in(key, 7)
    key_ids = jax.random.fold_in(base, 0)
    key_centers = jax.random.fold_in(base, 1)
    key_noise = jax.random.fold_in(base, 2)
    key_kind = jax.random.fold_in(base, 4)
    half_count = max(CLUSTERS // 2, 1)
    global_labels = jax.random.randint(key_ids, (POINTS,), 0, half_count)
    positions = jnp.arange(POINTS, dtype=jnp.int32)
    local_labels = CLUSTERS - half_count + positions * half_count // POINTS
    local_labels = jnp.minimum(local_labels, CLUSTERS - 1)
    kind = jax.random.randint(key_kind, (POINTS,), 0, 2)
    labels = jnp.where(kind == 1, local_labels, global_labels)
    centers = jnp.clip(jax.random.normal(key_centers, (CLUSTERS, F), jnp.float32), -4.0, 4.0)
    chosen = centers[labels]
    noise = 0.5 * jnp.clip(jax.random.normal(key_noise, (POINTS, F), jnp.float32), -4.0, 4.0)
    return (chosen + noise).astype(jnp.bfloat16)


def draw_vector(key, part):
    base = jax.random.fold_in(key, 11)
    rising = jnp.arange(POINTS, dtype=jnp.float32) / POINTS
    factor = jnp.exp(jax.random.uniform(base, (POINTS,), jnp.float32, jnp.log(0.1), jnp.log(10.0)))
    return factor * jnp.exp(jnp.log(10.0) * rising)


def setup_inputs(seed: int = 0, part: int = 0) -> dict:
    arg_keys = jax.random.split(jax.random.key(seed), 3)
    part_splits = jax.random.split(jax.random.fold_in(arg_keys[2], part), 3)
    return {
        "features": draw_features(jax.random.fold_in(jax.random.fold_in(arg_keys[2], part), 71), part),
        "vector": draw_vector(jax.random.fold_in(jax.random.fold_in(arg_keys[2], part), 71), part),
    }


def reference(features, vector):
    widened = features.astype(jnp.float32)
    unit_rows = (widened * lax.rsqrt(lax.optimization_barrier(jnp.mean(widened * widened, axis=1, keepdims=True)) + 1e-06) * (1.0 / math.sqrt(F))).astype(jnp.bfloat16)
    all_unit = unit_rows.astype(jnp.float32)
    block_len = math.gcd(POINTS, 512)
    blocks = POINTS // block_len
    stacked = all_unit.reshape(blocks, block_len, F)
    squarings = POWER.bit_length() - 1

    def one_block(block_rows):
        cosine = jnp.dot(block_rows, all_unit.T, precision=lax.Precision.HIGHEST)
        affinity = (1.0 + cosine) * 0.5
        for level in range(squarings):
            affinity = affinity * affinity
        weighted = jnp.dot(affinity, vector, precision=lax.Precision.HIGHEST)
        return (weighted, lax.optimization_barrier(jnp.sum(affinity, axis=1)))
    weighted, degree = lax.map(one_block, stacked)
    weighted = weighted.reshape(POINTS)
    degree = degree.reshape(POINTS)
    averaged = weighted / degree
    mean_abs = jnp.mean(jnp.abs(averaged)) + 1e-06
    return (averaged / mean_abs, degree / POINTS)
```

```python
import functools
import math

import jax
import jax.numpy as jnp
from jax import lax
from jax.experimental import pallas as pl
from jax.experimental.pallas import tpu as pltpu
from jax.sharding import PartitionSpec as P

POWER = 16
AXES = ("blk", "cols", "sub")
PAD = 16
BULKS = 1
WIDE = 256
TALL = 256
DEPTH = 3
LATE = 3
EACH = ((1, 0, 0), (0, 1, 0))
VMEM = pl.BlockSpec(memory_space=pltpu.VMEM)
HBM = pl.BlockSpec(memory_space=pltpu.HBM)


def power(base):
    for _ in range(POWER.bit_length() - 1):
        base = base * base
    return base


def fold_block(row_feats, totals, col_feats, col_vals):
    cosine = lax.dot_general(
        row_feats, col_feats, (((1,), (1,)), ((), ())), preferred_element_type=jnp.float32
    )
    affinity = power((1.0 + cosine) * 0.5)
    weighted = totals[0] + jnp.dot(affinity, col_vals, precision=lax.Precision.HIGHEST)
    degree = totals[1] + jnp.sum(affinity, axis=1)
    return (weighted, degree)


def sweep(row_feats, totals, pieces):
    col_feats, col_vals = pieces
    columns = col_feats.shape[0]
    block_len = math.gcd(columns, 512)
    blocks = columns // block_len
    if blocks == 1:
        return fold_block(row_feats, totals, col_feats, col_vals)
    stacked = (
        col_feats.reshape(blocks, block_len, col_feats.shape[1]),
        col_vals.reshape(blocks, block_len),
    )

    def advance(running, member):
        return (fold_block(row_feats, running, member[0], member[1]), None)

    result, _ = lax.scan(advance, totals, stacked)
    return result


def reduced(features, vector):
    own_rows = features.shape[0]
    half_rows = own_rows // 2
    gathered = lax.all_gather(features, "sub", axis=1, tiled=True)
    widened = gathered.astype(jnp.float32)
    unit_rows = (
        widened
        * lax.rsqrt(jnp.mean(widened * widened, axis=1, keepdims=True) + 1e-06)
        * (1.0 / math.sqrt(widened.shape[1]))
    ).astype(jnp.bfloat16)
    sub_index = lax.axis_index("sub")
    col_feats = lax.dynamic_slice_in_dim(unit_rows, sub_index * half_rows, half_rows, 0)
    col_vals = lax.dynamic_slice_in_dim(vector, sub_index * half_rows, half_rows, 0)
    points = own_rows * lax.axis_size("blk") * lax.axis_size("cols")
    block_feats = lax.all_gather(unit_rows, "cols", axis=0, tiled=True)
    zeros = jnp.zeros((block_feats.shape[0],), jnp.float32)
    partial_sums = sweep(
        block_feats,
        (zeros, zeros),
        (
            lax.all_gather(col_feats, "blk", axis=0, tiled=True),
            lax.all_gather(col_vals.astype(jnp.bfloat16), "blk", axis=0, tiled=True).astype(
                jnp.float32
            ),
        ),
    )
    block_weighted, block_degree = lax.psum((partial_sums[0], partial_sums[1]), ("cols", "sub"))
    block_averaged = block_weighted / block_degree
    total = lax.psum(jnp.sum(jnp.abs(block_averaged)), "blk")
    first_row = lax.axis_index("cols") * own_rows
    averaged = lax.dynamic_slice_in_dim(block_averaged, first_row, own_rows, 0)
    degree = lax.dynamic_slice_in_dim(block_degree, first_row, own_rows, 0)
    mean_abs = total / points + 1e-06
    return (averaged / mean_abs, degree / points)


def swap(x, *masks):
    sizes = [lax.axis_size(axis) for axis in AXES]
    place = lambda b, c, s: (b * sizes[1] + c) * sizes[2] + s
    pairs = [
        (place(b, c, s), place(*(at ^ mask for at, mask in zip((b, c, s), masks[s % len(masks)]))))
        for b in range(sizes[0])
        for c in range(sizes[1])
        for s in range(sizes[2])
    ]
    return lax.ppermute(x, AXES, pairs)


def pack(features, vector, packed, row, sems):
    rows = features.shape[0]
    size = rows // BULKS
    bulk = [
        pltpu.make_async_copy(
            features.at[k * size : (k + 1) * size], packed.at[k * size : (k + 1) * size], sems.at[k]
        )
        for k in range(BULKS)
    ]
    line = pltpu.make_async_copy(vector, row, sems.at[BULKS])
    line.start()
    for copy in bulk:
        copy.start()
    line.wait()
    value = row[...]
    high = value.astype(jnp.bfloat16)
    low = (value - high.astype(jnp.float32)).astype(jnp.bfloat16)
    rest = jnp.zeros((PAD - 2 * row.shape[0], row.shape[1]), jnp.bfloat16)
    packed[rows : rows + PAD, :] = jnp.concatenate([high, low, rest])
    for copy in bulk:
        copy.wait()


def admit(mine, base, theirs, twin, rows, unit, weights, at):
    half = mine.shape[1]
    width = 2 * half
    lines = rows // half
    a = mine[base : base + rows, :].astype(jnp.float32)
    b = theirs[twin : twin + rows, :].astype(jnp.float32)
    scale = lax.rsqrt(jnp.sum(a * a + b * b, axis=1, keepdims=True) / width + 1e-06)
    scale = scale * (1.0 / math.sqrt(width))
    unit[at : at + rows, :half] = (a * scale).astype(jnp.bfloat16)
    unit[at : at + rows, half:] = (b * scale).astype(jnp.bfloat16)
    tail = mine[base + rows : base + rows + PAD, :].astype(jnp.float32)
    for line in range(lines):
        span = slice(at + line * half, at + (line + 1) * half)
        weights[0:1, span] = tail[line : line + 1, :]
        weights[1:2, span] = tail[lines + line : lines + line + 1, :]
    ones = lax.broadcasted_iota(jnp.int32, (6, rows), 0) == 0
    weights[2:8, at : at + rows] = jnp.where(ones, 1.0, 0.0)


def product(left, right):
    return lax.dot_general(
        left, right, (((1,), (1,)), ((), ())), preferred_element_type=jnp.float32
    )


def step(rows, olds, slots, last, *refs):
    refs = list(refs)
    old = [refs[3 * k : 3 * k + 3] for k in range(olds)]
    count = 1 + max(max(i, j) for i, base, j, twin in slots)
    given, outs = refs[3 * olds : 3 * olds + count], refs[3 * olds + count :]
    if last:
        new_ref, mean_ref, unit, weights, results, sems = outs
        sums, old_sums = None, None
    else:
        unit, weights, sums = outs[:3]
        old_sums = outs[3:]
    fresh = 0
    for i, base, j, twin in slots:
        admit(given[i], base * (rows + PAD), given[j], twin * (rows + PAD), rows, unit, weights, fresh)
        fresh += rows
    names = [block[0] for block in old] + [unit]
    lines = [block[1][...].astype(jnp.bfloat16) for block in old] + [weights[...].astype(jnp.bfloat16)]
    here = len(old)
    tiles = []
    for k, block in enumerate(old):
        size = block[0].shape[0]
        for j in range(0, size, WIDE):
            tiles += [
                (at, min(at + TALL, fresh), k, j, min(j + WIDE, size)) for at in range(0, fresh, TALL)
            ]
    for at in range(0, fresh, rows):
        tiles += [(at, at + rows, here, j, min(j + WIDE, at)) for j in range(0, at, WIDE)]
        tiles += [(at, at + rows, here, at, at + rows)]
    columns, along, cosines, affinities = {}, {}, [], []

    def fold(table, key, value):
        table[key] = table[key] + value if key in table else value

    def add(tile, value):
        at, stop, k, j, end = tile
        found = jnp.dot(lines[here][:, at:stop], value, preferred_element_type=jnp.float32)
        for c in range(j, end, rows):
            fold(columns, (k, c), found[:, c - j : c - j + rows])
        if (k, j) != (here, at):
            found = product(value, lines[k][:, j:end])
            for r in range(at, stop, rows):
                fold(along, r, found[r - at : r - at + rows, :])

    for tile in tiles + [None] * (DEPTH + LATE + 2):
        if tile:
            at, stop, k, j, end = tile
            cosines.append((tile, product(unit[at:stop, :], names[k][j:end, :])))
        if cosines and (len(cosines) > DEPTH or not tile):
            done, value = cosines.pop(0)
            affinities.append((done, power(1.0 + value).astype(jnp.bfloat16)))
        if affinities and (len(affinities) > LATE or not (tile or cosines)):
            add(*affinities.pop(0))
    assert not cosines and not affinities
    for at, value in along.items():
        fold(columns, (here, at), value.T)

    def joined(k, size):
        return jnp.concatenate([columns[k, c] for c in range(0, size, rows)], axis=1)

    totals = [block[2][...] + joined(k, block[0].shape[0]) for k, block in enumerate(old)]
    total = joined(here, fresh)
    if not last:
        sums[...] = total
        for ref, value in zip(old_sums, totals):
            ref[...] = value
        return
    points = fresh + sum(block[0].shape[0] for block in old)
    leave = [
        pltpu.make_async_copy(results.at[k : k + 1], ref, sems.at[k])
        for k, ref in enumerate((new_ref, mean_ref))
    ]
    results[1:2, :] = totals[0][2:3, :rows] * (0.5**POWER / points)
    leave[1].start()
    averaged = [(t[0:1] + t[1:2]) / t[2:3] for t in totals + [total]]
    mean_abs = sum(jnp.sum(jnp.abs(a)) for a in averaged) / points + 1e-06
    results[0:1, :] = averaged[0][:, :rows] / mean_abs
    leave[0].start()
    for copy in leave:
        copy.wait()


def gathered(features, vector):
    rows, half = features.shape
    lines = rows // half
    shape = jax.ShapeDtypeStruct
    far_blk = lax.axis_size("blk") // 2
    params = pltpu.CompilerParams(vmem_limit_bytes=24 * 2**20)

    def advance(blocks, given, slots, last=False):
        fresh = len(slots) * rows
        unit, weights = shape((fresh, 2 * half), jnp.bfloat16), shape((8, fresh), jnp.float32)
        done = sum(block[0].shape[0] for block in blocks)
        outs = [unit, weights, weights] + [shape(block[2].shape, jnp.float32) for block in blocks]
        scratch = []
        if last:
            outs = [shape((1, rows), jnp.float32)] * 2
            scratch = [pltpu.VMEM(x.shape, x.dtype) for x in (unit, weights)]
            scratch += [pltpu.VMEM((2, rows), jnp.float32), pltpu.SemaphoreType.DMA((2,))]
        inputs = [x for block in blocks for x in block] + given
        work = 2 * 2 * half * fresh * (fresh + done)
        result = pl.pallas_call(
            functools.partial(step, rows, len(blocks), slots, last),
            out_shape=outs,
            in_specs=[VMEM] * len(inputs),
            out_specs=[HBM if last else VMEM] * len(outs),
            scratch_shapes=scratch,
            compiler_params=params,
            cost_estimate=pl.CostEstimate(flops=work, bytes_accessed=0, transcendentals=0),
        )(*inputs)
        if last:
            return result
        return [(b[0], b[1], s) for b, s in zip(blocks, result[3:])] + [tuple(result[:3])]

    place = pltpu.with_memory_space_constraint
    own = pl.pallas_call(
        pack,
        out_shape=pltpu.VMEM((rows + PAD, half), jnp.bfloat16),
        in_specs=[HBM, HBM],
        out_specs=VMEM,
        scratch_shapes=[pltpu.VMEM((lines, half), jnp.float32), pltpu.SemaphoreType.DMA((BULKS + 1,))],
        compiler_params=params,
        name="pack",
    )(place(features, pltpu.HBM), place(vector.reshape(lines, half), pltpu.HBM))
    other, both, each = (0, 0, 1), (1, 1, 0), EACH
    far = swap(own, (far_blk, 0, 0))
    own2 = swap(own, other)
    dn = swap(own, both)
    na = swap(jnp.concatenate([own, own2]), *each)
    far2 = swap(far, other)
    df = swap(far, both)
    fa = swap(jnp.concatenate([far, far2]), *each)
    dn2 = swap(dn, other)
    na2 = swap(na, other)
    df2 = swap(df, other)
    fa2 = swap(fa, other)
    blocks = advance([], [own, own2, far, far2], [(0, 0, 1, 0), (2, 0, 3, 0)])
    blocks = advance(blocks, [na, dn, dn2], [(0, 0, 0, 1), (1, 0, 2, 0)])
    blocks = advance(blocks, [na2], [(0, 1, 0, 0)])
    blocks = advance(blocks, [df, df2, fa], [(0, 0, 1, 0), (2, 0, 2, 1)])
    new, mean = advance(blocks, [fa2], [(0, 1, 0, 0)], True)
    return new.reshape(rows), mean.reshape(rows)


def solution(mesh):
    in_specs = (P(("groups", "blk", "cols"), "sub"), P(("groups", "blk", "cols")))
    out_specs = (P(("groups", "blk", "cols")), P(("groups", "blk", "cols")))
    few = (mesh.shape["blk"], mesh.shape["cols"], mesh.shape["sub"]) == (4, 2, 2)
    return jax.shard_map(
        gathered if few else reduced,
        mesh=mesh,
        in_specs=in_specs,
        out_specs=out_specs,
        check_vma=False,
    )
```

```python
import functools
import math

import jax
import jax.numpy as jnp
from jax import lax
from jax.experimental import pallas as pl
from jax.experimental.pallas import tpu as pltpu
from jax.sharding import PartitionSpec as P

POWER = 16
AXES = ("blk", "cols", "sub")
PAD = 8
BULKS = 1
WIDE = 256
TALL = 256
DEPTH = 20
LATE = 20
EACH = ((1, 0, 0), (0, 1, 0))
VMEM = pl.BlockSpec(memory_space=pltpu.VMEM)
HBM = pl.BlockSpec(memory_space=pltpu.HBM)


def power(base):
    for _ in range(POWER.bit_length() - 1):
        base = base * base
    return base


def fold_block(row_feats, totals, col_feats, col_vals):
    cosine = lax.dot_general(
        row_feats, col_feats, (((1,), (1,)), ((), ())), preferred_element_type=jnp.float32
    )
    affinity = power((1.0 + cosine) * 0.5)
    weighted = totals[0] + jnp.dot(affinity, col_vals, precision=lax.Precision.HIGHEST)
    degree = totals[1] + jnp.sum(affinity, axis=1)
    return (weighted, degree)


def sweep(row_feats, totals, pieces):
    col_feats, col_vals = pieces
    columns = col_feats.shape[0]
    block_len = math.gcd(columns, 512)
    blocks = columns // block_len
    if blocks == 1:
        return fold_block(row_feats, totals, col_feats, col_vals)
    stacked = (
        col_feats.reshape(blocks, block_len, col_feats.shape[1]),
        col_vals.reshape(blocks, block_len),
    )

    def advance(running, member):
        return (fold_block(row_feats, running, member[0], member[1]), None)

    result, _ = lax.scan(advance, totals, stacked)
    return result


def reduced(features, vector):
    own_rows = features.shape[0]
    half_rows = own_rows // 2
    gathered = lax.all_gather(features, "sub", axis=1, tiled=True)
    widened = gathered.astype(jnp.float32)
    unit_rows = (
        widened
        * lax.rsqrt(jnp.mean(widened * widened, axis=1, keepdims=True) + 1e-06)
        * (1.0 / math.sqrt(widened.shape[1]))
    ).astype(jnp.bfloat16)
    sub_index = lax.axis_index("sub")
    col_feats = lax.dynamic_slice_in_dim(unit_rows, sub_index * half_rows, half_rows, 0)
    col_vals = lax.dynamic_slice_in_dim(vector, sub_index * half_rows, half_rows, 0)
    points = own_rows * lax.axis_size("blk") * lax.axis_size("cols")
    block_feats = lax.all_gather(unit_rows, "cols", axis=0, tiled=True)
    zeros = jnp.zeros((block_feats.shape[0],), jnp.float32)
    partial_sums = sweep(
        block_feats,
        (zeros, zeros),
        (
            lax.all_gather(col_feats, "blk", axis=0, tiled=True),
            lax.all_gather(col_vals.astype(jnp.bfloat16), "blk", axis=0, tiled=True).astype(
                jnp.float32
            ),
        ),
    )
    block_weighted, block_degree = lax.psum((partial_sums[0], partial_sums[1]), ("cols", "sub"))
    block_averaged = block_weighted / block_degree
    total = lax.psum(jnp.sum(jnp.abs(block_averaged)), "blk")
    first_row = lax.axis_index("cols") * own_rows
    averaged = lax.dynamic_slice_in_dim(block_averaged, first_row, own_rows, 0)
    degree = lax.dynamic_slice_in_dim(block_degree, first_row, own_rows, 0)
    mean_abs = total / points + 1e-06
    return (averaged / mean_abs, degree / points)


def swap(x, *masks):
    sizes = [lax.axis_size(axis) for axis in AXES]
    place = lambda b, c, s: (b * sizes[1] + c) * sizes[2] + s
    pairs = [
        (place(b, c, s), place(*(at ^ mask for at, mask in zip((b, c, s), masks[s % len(masks)]))))
        for b in range(sizes[0])
        for c in range(sizes[1])
        for s in range(sizes[2])
    ]
    return lax.ppermute(x, AXES, pairs)


def pack(features, vector, packed, row, sems):
    rows = features.shape[0]
    size = rows // BULKS
    bulk = [
        pltpu.make_async_copy(
            features.at[k * size : (k + 1) * size], packed.at[k * size : (k + 1) * size], sems.at[k]
        )
        for k in range(BULKS)
    ]
    line = pltpu.make_async_copy(vector, row, sems.at[BULKS])
    line.start()
    for copy in bulk:
        copy.start()
    line.wait()
    value = row[...]
    high = value.astype(jnp.bfloat16)
    low = (value - high.astype(jnp.float32)).astype(jnp.bfloat16)
    rest = jnp.zeros((PAD - 2 * row.shape[0], row.shape[1]), jnp.bfloat16)
    packed[rows : rows + PAD, :] = jnp.concatenate([high, low, rest])
    for copy in bulk:
        copy.wait()


def admit(mine, base, theirs, twin, rows, unit, weights, at):
    half = mine.shape[1]
    width = 2 * half
    lines = rows // half
    a = mine[base : base + rows, :].astype(jnp.float32)
    b = theirs[twin : twin + rows, :].astype(jnp.float32)
    scale = lax.rsqrt(jnp.sum(a * a + b * b, axis=1, keepdims=True) / width + 1e-06)
    scale = scale * (1.0 / math.sqrt(width))
    unit[at : at + rows, :half] = (a * scale).astype(jnp.bfloat16)
    unit[at : at + rows, half:] = (b * scale).astype(jnp.bfloat16)
    tail = mine[base + rows : base + rows + PAD, :].astype(jnp.float32)
    for line in range(lines):
        span = slice(at + line * half, at + (line + 1) * half)
        weights[0:1, span] = tail[line : line + 1, :]
        weights[1:2, span] = tail[lines + line : lines + line + 1, :]
    ones = lax.broadcasted_iota(jnp.int32, (6, rows), 0) == 0
    weights[2:8, at : at + rows] = jnp.where(ones, 1.0, 0.0)


def product(left, right):
    return lax.dot_general(
        left, right, (((1,), (1,)), ((), ())), preferred_element_type=jnp.float32
    )


def step(rows, olds, slots, last, *refs):
    refs = list(refs)
    old = [refs[3 * k : 3 * k + 3] for k in range(olds)]
    count = 1 + max(max(i, j) for i, base, j, twin in slots)
    given, outs = refs[3 * olds : 3 * olds + count], refs[3 * olds + count :]
    if last:
        new_ref, mean_ref, unit, weights, results, sems = outs
        sums, old_sums = None, None
    else:
        unit, weights, sums = outs[:3]
        old_sums = outs[3:]
    fresh = 0
    for i, base, j, twin in slots:
        admit(given[i], base * (rows + PAD), given[j], twin * (rows + PAD), rows, unit, weights, fresh)
        fresh += rows
    names = [block[0] for block in old] + [unit]
    lines = [block[1][...].astype(jnp.bfloat16) for block in old] + [weights[...].astype(jnp.bfloat16)]
    here = len(old)
    tiles = []
    for k, block in enumerate(old):
        size = block[0].shape[0]
        for j in range(0, size, WIDE):
            tiles += [
                (at, min(at + TALL, fresh), k, j, min(j + WIDE, size)) for at in range(0, fresh, TALL)
            ]
    for at in range(0, fresh, rows):
        tiles += [(at, at + rows, here, j, min(j + WIDE, at)) for j in range(0, at, WIDE)]
        tiles += [(at, at + rows, here, at, at + rows)]
    columns, along, cosines, affinities = {}, {}, [], []

    def fold(table, key, value):
        table[key] = table[key] + value if key in table else value

    def add(tile, value):
        at, stop, k, j, end = tile
        found = jnp.dot(lines[here][:, at:stop], value, preferred_element_type=jnp.float32)
        for c in range(j, end, rows):
            fold(columns, (k, c), found[:, c - j : c - j + rows])
        if (k, j) != (here, at):
            found = product(value, lines[k][:, j:end])
            for r in range(at, stop, rows):
                fold(along, r, found[r - at : r - at + rows, :])

    for tile in tiles + [None] * (DEPTH + LATE + 2):
        if tile:
            at, stop, k, j, end = tile
            cosines.append((tile, product(unit[at:stop, :], names[k][j:end, :])))
        if cosines and (len(cosines) > DEPTH or not tile):
            done, value = cosines.pop(0)
            affinities.append((done, power(1.0 + value).astype(jnp.bfloat16)))
        if affinities and (len(affinities) > LATE or not (tile or cosines)):
            add(*affinities.pop(0))
    assert not cosines and not affinities
    for at, value in along.items():
        fold(columns, (here, at), value.T)

    def joined(k, size):
        return jnp.concatenate([columns[k, c] for c in range(0, size, rows)], axis=1)

    totals = [block[2][...] + joined(k, block[0].shape[0]) for k, block in enumerate(old)]
    total = joined(here, fresh)
    if not last:
        sums[...] = total
        for ref, value in zip(old_sums, totals):
            ref[...] = value
        return
    points = fresh + sum(block[0].shape[0] for block in old)
    leave = [
        pltpu.make_async_copy(results.at[k : k + 1], ref, sems.at[k])
        for k, ref in enumerate((new_ref, mean_ref))
    ]
    results[1:2, :] = totals[0][2:3, :rows] * (0.5**POWER / points)
    leave[1].start()
    averaged = [(t[0:1] + t[1:2]) / t[2:3] for t in totals + [total]]
    mean_abs = sum(jnp.sum(jnp.abs(a)) for a in averaged) / points + 1e-06
    results[0:1, :] = averaged[0][:, :rows] / mean_abs
    leave[0].start()
    for copy in leave:
        copy.wait()


def gathered(features, vector):
    rows, half = features.shape
    lines = rows // half
    shape = jax.ShapeDtypeStruct
    far_blk = lax.axis_size("blk") // 2
    params = pltpu.CompilerParams(vmem_limit_bytes=24 * 2**20)

    def advance(blocks, given, slots, last=False):
        fresh = len(slots) * rows
        unit, weights = shape((fresh, 2 * half), jnp.bfloat16), shape((8, fresh), jnp.float32)
        done = sum(block[0].shape[0] for block in blocks)
        outs = [unit, weights, weights] + [shape(block[2].shape, jnp.float32) for block in blocks]
        scratch = []
        if last:
            outs = [shape((1, rows), jnp.float32)] * 2
            scratch = [pltpu.VMEM(x.shape, x.dtype) for x in (unit, weights)]
            scratch += [pltpu.VMEM((2, rows), jnp.float32), pltpu.SemaphoreType.DMA((2,))]
        inputs = [x for block in blocks for x in block] + given
        work = 2 * 2 * half * fresh * (fresh + done)
        result = pl.pallas_call(
            functools.partial(step, rows, len(blocks), slots, last),
            out_shape=outs,
            in_specs=[VMEM] * len(inputs),
            out_specs=[HBM if last else VMEM] * len(outs),
            scratch_shapes=scratch,
            compiler_params=params,
            cost_estimate=pl.CostEstimate(flops=work, bytes_accessed=0, transcendentals=0),
        )(*inputs)
        if last:
            return result
        return [(b[0], b[1], s) for b, s in zip(blocks, result[3:])] + [tuple(result[:3])]

    place = pltpu.with_memory_space_constraint
    own = pl.pallas_call(
        pack,
        out_shape=pltpu.VMEM((rows + PAD, half), jnp.bfloat16),
        in_specs=[HBM, HBM],
        out_specs=VMEM,
        scratch_shapes=[pltpu.VMEM((lines, half), jnp.float32), pltpu.SemaphoreType.DMA((BULKS + 1,))],
        compiler_params=params,
        name="pack",
    )(place(features, pltpu.HBM), place(vector.reshape(lines, half), pltpu.HBM))
    other, both, each = (0, 0, 1), (1, 1, 0), EACH
    far = swap(own, (far_blk, 0, 0))
    own2 = swap(own, other)
    dn = swap(own, both)
    na = swap(jnp.concatenate([own, own2]), *each)
    far2 = swap(far, other)
    df = swap(far, both)
    fa = swap(jnp.concatenate([far, far2]), *each)
    dn2 = swap(dn, other)
    na2 = swap(na, other)
    df2 = swap(df, other)
    fa2 = swap(fa, other)
    blocks = advance([], [own, own2, far, far2], [(0, 0, 1, 0), (2, 0, 3, 0)])
    blocks = advance(blocks, [na, dn, dn2], [(0, 0, 0, 1), (1, 0, 2, 0)])
    blocks = advance(blocks, [na2], [(0, 1, 0, 0)])
    blocks = advance(blocks, [df, df2, fa], [(0, 0, 1, 0), (2, 0, 2, 1)])
    new, mean = advance(blocks, [fa2], [(0, 1, 0, 0)], True)
    return new.reshape(rows), mean.reshape(rows)


def solution(mesh):
    in_specs = (P(("groups", "blk", "cols"), "sub"), P(("groups", "blk", "cols")))
    out_specs = (P(("groups", "blk", "cols")), P(("groups", "blk", "cols")))
    few = (mesh.shape["blk"], mesh.shape["cols"], mesh.shape["sub"]) == (4, 2, 2)
    return jax.shard_map(
        gathered if few else reduced,
        mesh=mesh,
        in_specs=in_specs,
        out_specs=out_specs,
        check_vma=False,
    )
```
